32 devices in a mesh: pts: 8 (over y, x, core), wlk: 4 (over z).
Axes of the slice: x: 2, y: 2, z: 4, core: 2. Of those that a mesh axis runs over, the one named last changes fastest.
Arguments:
- green_half: bfloat16 [8, 400, 2400], P('wlk'), may hold values from -6 to 6
- collocation: bfloat16 [2400, 9600], P('wlk', 'pts'), may hold values from -0.125 to 0.125
- occupied: bfloat16 [9600, 400], P('pts'), may hold values from -0.0029296875 to 0.0029296875
- kernel: bfloat16 [9600, 9600], P('pts'), may hold values from 0 to 16, as said below
Outputs:
- potential: float32 [8, 9600], P('wlk', 'pts')
- coulomb_energy: float32 [8], P('wlk')
- exchange_energy: float32 [8], P('wlk')
The draws below stay inside these ranges and needn't reach their ends.
Inputs may be any that keep to these rules, and one draw needn't show every extreme that they name: kernel is symmetric and positive definite: kernel[p, q] equals kernel[q, p].
All inputs are finite; a program needn't handle non-finite values.
Results may differ from the reference program's by a relative error of at most 0.008.
Values may be sent and summed in bfloat16 or wider, within the bound.
A program may use at most 192 MiB of HBM per device.

```python
import jax
import jax.numpy as jnp
from jax import lax

ORB = 2400
ELEC = 400
RANK = 9600
W = 8


def draw_kernel(key, part):
    point_spots = jax.random.uniform(jax.random.fold_in(key, 3), (RANK, 3), jnp.float32, 0.0, 1.0)
    length = (10.0 / RANK) ** (1.0 / 3.0)
    squared = jnp.zeros((RANK, RANK), jnp.float32)
    for column in range(3):
        offset = point_spots[:, column][:, None] - point_spots[:, column][None, :]
        squared = squared + offset * offset
    distance = jnp.sqrt(squared)
    values = 6.0 * jnp.exp(-distance / length) + 1.5 * jnp.eye(RANK, dtype=jnp.float32)
    return values.astype(jnp.bfloat16)


def block_scale(own_key, extent, split, smallest, largest):
    level, own = 1.0, jax.random.fold_in(own_key, 6)
    for axis_at, shards_of in split:
        draws = jnp.exp(jax.random.uniform(jax.random.fold_in(own, axis_at), (shards_of,), jnp.float32, smallest / len(split), largest / len(split)))
        level = level * jnp.repeat(draws, extent[axis_at] // shards_of).reshape([-1 if axis == axis_at else 1 for axis in range(len(extent))])
    return level


def noise(rng, shape, scale, limit, split=(), held_as=jnp.bfloat16):
    values = scale * jax.random.normal(rng, shape, jnp.float32)
    if split:
        values = values * block_scale(rng, shape, split, -0.22, 0.18)
    return jnp.clip(values, -limit, limit).astype(held_as)


def setup_inputs(seed: int = 0) -> dict:
    arg_keys = jax.random.split(jax.random.key(seed), 5)
    return {
        "green_half": noise(arg_keys[0], (W, ELEC, ORB), 1.0, 6.0, ((0, 4),)),
        "collocation": noise(arg_keys[1], (ORB, RANK), ORB ** -0.5, 0.125, ((0, 4), (1, 8))),
        "occupied": noise(arg_keys[2], (RANK, ELEC), (RANK * ELEC) ** -0.5, 0.0029296875, ((0, 8),)),
        "kernel": draw_kernel(jax.random.fold_in(arg_keys[4], 71), 0),
    }


def reference(green_half, collocation, occupied, kernel):
    kernel_float = kernel.astype(jnp.float32)

    def one_walker(green_one):
        theta = jnp.dot(green_one, collocation, preferred_element_type=jnp.float32).astype(jnp.bfloat16)
        density = jnp.sum(theta.astype(jnp.float32) * occupied.T.astype(jnp.float32), axis=0)
        density_b = density.astype(jnp.bfloat16)
        potential = jnp.dot(kernel, density_b, preferred_element_type=jnp.float32)
        coulomb = 0.5 * jnp.sum(density * potential)
        cross = jnp.dot(theta.T, occupied.T, preferred_element_type=jnp.float32)
        exchange = -0.5 * jnp.sum(kernel_float * cross * cross.T)
        return potential, coulomb, exchange

    potential, coulomb, exchange = lax.map(one_walker, green_half)
    return potential, coulomb, exchange
```

```python
import functools

import jax
import jax.numpy as jnp
from jax import lax
from jax.experimental import pallas as pl
from jax.experimental.pallas import tpu as pltpu
from jax.sharding import PartitionSpec as P

NT = (((1,), (1,)), ((), ()))


def tile_of(points):
    return max(t for t in range(8, 257, 8) if points % t == 0)


def exchange_kernel(walkers, first_ref, near_ref, occ_near_ref, far_ref, occ_far_ref, k_ref, out_ref):
    @pl.when(pl.program_id(0) == 0)
    def _():
        out_ref[...] = jnp.zeros_like(out_ref)

    rows = occ_near_ref.shape[0]
    width = k_ref.shape[2]
    kern = k_ref[0].astype(jnp.float32)
    for w in range(walkers):
        near = lax.dot_general(near_ref[w], occ_far_ref[...], NT, preferred_element_type=jnp.float32)
        far = lax.dot_general(occ_near_ref[...], far_ref[w], NT, preferred_element_type=jnp.float32)
        out_ref[w] += jnp.sum((kern * near * far).reshape(rows // 8, 8, width), axis=0)


def exchange_block(first_tile, theta, occupied, theta_far, occ_far, tiles):
    walkers, rows, elec = theta.shape
    width = tiles.shape[2]
    steps = occ_far.shape[0] // width
    out = pl.pallas_call(
        functools.partial(exchange_kernel, walkers),
        out_shape=jax.ShapeDtypeStruct((walkers, 8, width), jnp.float32),
        grid_spec=pltpu.PrefetchScalarGridSpec(
            num_scalar_prefetch=1,
            grid=(steps,),
            in_specs=[
                pl.BlockSpec((walkers, rows, elec), lambda j, s: (0, 0, 0)),
                pl.BlockSpec((rows, elec), lambda j, s: (0, 0)),
                pl.BlockSpec((walkers, width, elec), lambda j, s: (0, j, 0)),
                pl.BlockSpec((width, elec), lambda j, s: (j, 0)),
                pl.BlockSpec((1, rows, width), lambda j, s: (s[0] + j, 0, 0)),
            ],
            out_specs=pl.BlockSpec((walkers, 8, width), lambda j, s: (0, 0, 0)),
        ),
        compiler_params=pltpu.CompilerParams(vmem_limit_bytes=48 * 1024 * 1024),
        cost_estimate=pl.CostEstimate(
            flops=2 * walkers * 2 * rows * occ_far.shape[0] * elec * 2,
            bytes_accessed=2 * rows * occ_far.shape[0],
            transcendentals=0,
        ),
        name="exchange",
    )(first_tile.reshape(1).astype(jnp.int32), theta, occupied, theta_far, occ_far, tiles)
    return jnp.sum(out, axis=(1, 2))


def shifted(block, distance):
    devices = lax.axis_size("pts")
    return lax.ppermute(block, "pts", [((i - distance) % devices, i) for i in range(devices)])


def local(green_half, collocation, occupied, kernel):
    rows, elec = occupied.shape
    devices = lax.axis_size("pts")
    position = lax.axis_index("pts")
    width = tile_of(rows)
    per_block = rows // width
    first = (per_block + 1) // 2
    spans = ((0, first), (first, per_block))
    tiles = kernel.reshape(rows, kernel.shape[1] // width, width).transpose(1, 0, 2)
    far_counts = range(1, devices // 2 + 1)

    occ_far = {}
    travel = occupied
    for stride in far_counts:
        travel = shifted(travel, 1)
        occ_far[stride] = travel

    parts = []
    for low, high in spans:
        points = collocation[:, low * width : high * width]
        gathered = lax.all_gather(points, "wlk", axis=0, tiled=True)
        parts.append(
            jnp.einsum("mp,wim->wpi", gathered, green_half, preferred_element_type=jnp.float32).astype(
                jnp.bfloat16
            )
        )
    theta = jnp.concatenate(parts, axis=1)

    far_parts = [{}, {}]
    for h in range(2):
        travel = parts[h]
        for stride in far_counts:
            travel = shifted(travel, 1)
            far_parts[h][stride] = travel

    density = jnp.einsum("wpi,pi->wp", theta, occupied, preferred_element_type=jnp.float32)
    density_b = density.astype(jnp.bfloat16)
    density_all = lax.all_gather(density_b, "pts", axis=1, tiled=True)
    potential = jnp.einsum("wq,aq->wa", density_all, kernel, preferred_element_type=jnp.float32)

    exchange_sum = exchange_block(position * per_block, theta, occupied, theta, occupied, tiles)
    for h, (low, high) in enumerate(spans):
        for stride in far_counts:
            source = (position - stride) % devices
            weight = 1.0 if 2 * stride == devices else 2.0
            exchange_sum = exchange_sum + weight * exchange_block(
                source * per_block + low,
                theta,
                occupied,
                far_parts[h][stride],
                occ_far[stride][low * width : high * width],
                tiles,
            )
    coulomb = 0.5 * jnp.sum(density * potential, axis=1)
    coulomb_energy, exchange_energy = lax.psum((coulomb, -0.5 * exchange_sum), "pts")
    return (potential, coulomb_energy, exchange_energy)


def solution(mesh):
    placed = (P("wlk", None, None), P("wlk", "pts"), P("pts", None), P("pts", None))
    return jax.shard_map(
        local,
        mesh=mesh,
        in_specs=placed,
        out_specs=(P("wlk", "pts"), P("wlk"), P("wlk")),
        check_vma=False,
    )
```

```python
import functools

import jax
import jax.numpy as jnp
from jax import lax
from jax.experimental import pallas as pl
from jax.experimental.pallas import tpu as pltpu
from jax.sharding import PartitionSpec as P

TILE = 256


def exchange_kernel(walkers, limit, near_ref, occ_near_ref, far_ref, occ_far_ref, k_ref, out_ref):
    step = pl.program_id(0)

    @pl.when(step == 0)
    def _():
        out_ref[...] = jnp.zeros_like(out_ref)

    rows = occ_near_ref.shape[0]
    kern = k_ref[...].astype(jnp.float32)
    lane = step * TILE + lax.broadcasted_iota(jnp.int32, (8, TILE), 1)
    for w in range(walkers):
        near = jnp.dot(near_ref[w], occ_far_ref[...], preferred_element_type=jnp.float32)
        far = jnp.dot(occ_near_ref[...], far_ref[w], preferred_element_type=jnp.float32)
        term = jnp.sum((kern * near * far).reshape(rows // 8, 8, TILE), axis=0)
        out_ref[w] += jnp.where(lane < limit, term, 0.0)


def exchange_block(low, theta, occupied, far, occ_far, k_block):
    walkers, rows, elec = theta.shape
    points = far.shape[2]
    skip = low // TILE
    out = pl.pallas_call(
        functools.partial(exchange_kernel, walkers, points),
        out_shape=jax.ShapeDtypeStruct((walkers, 8, TILE), jnp.float32),
        grid=(pl.cdiv(points, TILE),),
        in_specs=[
            pl.BlockSpec((walkers, rows, elec), lambda j: (0, 0, 0)),
            pl.BlockSpec((rows, elec), lambda j: (0, 0)),
            pl.BlockSpec((walkers, elec, TILE), lambda j: (0, 0, j)),
            pl.BlockSpec((elec, TILE), lambda j: (0, skip + j)),
            pl.BlockSpec((rows, TILE), lambda j: (0, skip + j)),
        ],
        out_specs=pl.BlockSpec((walkers, 8, TILE), lambda j: (0, 0, 0)),
        compiler_params=pltpu.CompilerParams(vmem_limit_bytes=60 * 1024 * 1024),
        cost_estimate=pl.CostEstimate(
            flops=2 * walkers * 2 * rows * points * elec * 2,
            bytes_accessed=2 * rows * points,
            transcendentals=0,
        ),
        name="exchange",
    )(theta, occupied, far, occ_far, k_block)
    return jnp.sum(out, axis=(1, 2))


def shifted(block, distance):
    devices = lax.axis_size("pts")
    return lax.ppermute(block, "pts", [((i - distance) % devices, i) for i in range(devices)])


def local(green_half, collocation, occupied, kernel):
    rows, elec = occupied.shape
    devices = lax.axis_size("pts")
    position = lax.axis_index("pts")
    cut = pl.cdiv(pl.cdiv(rows, TILE), 2) * TILE
    spans = ((0, cut), (cut, rows))
    far_counts = range(1, devices // 2 + 1)

    occ_turned = occupied.T
    occ_far = {}
    travel = occ_turned
    for stride in far_counts:
        travel = shifted(travel, 1)
        occ_far[stride] = travel
    k_blocks = [
        lax.dynamic_slice_in_dim(kernel, ((position - stride) % devices) * rows, rows, 1)
        for stride in range(devices // 2 + 1)
    ]

    parts = []
    for low, high in spans:
        gathered = lax.all_gather(collocation[:, low:high], "wlk", axis=0, tiled=True)
        if low == 0:
            gathered, *k_blocks = lax.optimization_barrier((gathered, *k_blocks))
        parts.append(
            jnp.einsum("wim,mp->wip", green_half, gathered, preferred_element_type=jnp.float32).astype(
                jnp.bfloat16
            )
        )
    theta_turned = jnp.concatenate(parts, axis=2)
    theta = theta_turned.transpose(0, 2, 1)

    far_parts = [{}, {}]
    for h in range(2):
        travel = parts[h]
        for stride in far_counts:
            travel = shifted(travel, 1)
            far_parts[h][stride] = travel

    density = jnp.sum(
        theta_turned.astype(jnp.float32) * occ_turned.astype(jnp.float32)[None], axis=1
    )
    density_b = density.astype(jnp.bfloat16)
    density_all = lax.all_gather(density_b, "pts", axis=1, tiled=True)
    potential = jnp.einsum("wq,aq->wa", density_all, kernel, preferred_element_type=jnp.float32)

    exchange_sum = exchange_block(0, theta, occupied, theta_turned, occ_turned, k_blocks[0])
    for h, (low, high) in enumerate(spans):
        for stride in far_counts:
            weight = 1.0 if 2 * stride == devices else 2.0
            exchange_sum = exchange_sum + weight * exchange_block(
                low, theta, occupied, far_parts[h][stride], occ_far[stride], k_blocks[stride]
            )
    coulomb = 0.5 * jnp.sum(density * potential, axis=1)
    coulomb_energy, exchange_energy = lax.psum((coulomb, -0.5 * exchange_sum), "pts")
    return (potential, coulomb_energy, exchange_energy)


def solution(mesh):
    placed = (P("wlk", None, None), P("wlk", "pts"), P("pts", None), P("pts", None))
    return jax.shard_map(
        local,
        mesh=mesh,
        in_specs=placed,
        out_specs=(P("wlk", "pts"), P("wlk"), P("wlk")),
        check_vma=False,
    )
```
